32 devices in a mesh: node: 8 (over z, y), dev: 4 (over x, core).
Axes of the slice: x: 2, y: 2, z: 4, core: 2. Of those that a mesh axis runs over, the one named last changes fastest.
Arguments:
- tokens: bfloat16 [128, 5120], P(('node', 'dev')), may hold values from -6 to 6
- node_pick: int32 [128, 3], P(('node', 'dev')), may hold values from 0 to 7, as said below
- expert_pick: int32 [128, 6], P(('node', 'dev')), may hold values from 0 to 3, as said below
- gate_weight: bfloat16 [128, 6], P(('node', 'dev')), may hold values from 0.099609375 to 1
- w_gate: bfloat16 [24576, 5120], P(('node', 'dev')), may hold values from -0.078125 to 0.078125
- w_up: bfloat16 [24576, 5120], P(('node', 'dev')), may hold values from -0.078125 to 0.078125
- w_down: bfloat16 [24576, 5120], P(('node', 'dev')), may hold values from -0.21875 to 0.21875
Outputs:
- mixed_out: bfloat16 [128, 5120], P(('node', 'dev'))
The draws below stay inside these ranges and needn't reach their ends.
Inputs may be any that keep to these rules, and one draw needn't show every extreme that they name: `node_pick`: A token's three nodes differ. On every device at most 2 of its 4 tokens choose one node, and some node is chosen by exactly 2 of them. `expert_pick`: columns 2k and 2k + 1 name two different experts of node node_pick[t, k]. Among the tokens of all devices with one index along dev, at most 12 of those choosing one node pick one same expert of it; this is reached somewhere in every draw.
All inputs are finite; a program needn't handle non-finite values.
Results may differ from the reference program's by a relative error of at most 0.009.
Values may be sent and summed in bfloat16 or wider, within the bound.
A program may use at most 64 MiB of HBM per device.

```python
import math
import jax
import jax.numpy as jnp
from jax import lax

D = 5120
FF = 768
EXP_NODE = 4
TOK_DEV = 4
CYCLE = 6
CB = 12
EXPERTS = 32
TOKENS = 128
N_NODE = 8
N_DEV = 4


def routing(key):
    slot_count = 3 * TOK_DEV
    offset_keys = jax.random.split(jax.random.fold_in(key, 101), N_DEV)
    offsets = jax.vmap(lambda sub_key: jax.random.permutation(sub_key, N_NODE)[:CYCLE])(offset_keys)
    source = jnp.arange(N_NODE, dtype=jnp.int32)[:, None, None]
    slot_ids = jnp.arange(slot_count, dtype=jnp.int32) % CYCLE
    chosen = (source + offsets[None, :, slot_ids].astype(jnp.int32)) % N_NODE
    hot_local = jax.random.randint(jax.random.fold_in(key, 102), (N_NODE * N_DEV,), 0, EXP_NODE)
    hot_flag = jax.random.randint(jax.random.fold_in(key, 103), (N_NODE * N_DEV,), 0, 2)
    hot_flag = jnp.maximum(hot_flag, (jnp.arange(N_NODE * N_DEV) == 0).astype(jnp.int32))
    column = jnp.arange(N_DEV, dtype=jnp.int32)[None, :, None]
    receiver = chosen * N_DEV + column
    hot_here = hot_local[receiver]
    flag_here = hot_flag[receiver]
    shape = (N_NODE, N_DEV, slot_count)
    free_pick = jax.random.randint(jax.random.fold_in(key, 104), shape, 0, EXP_NODE)
    step_pick = jax.random.randint(jax.random.fold_in(key, 105), shape, 0, EXP_NODE - 1)
    first_pick = jnp.where(flag_here == 1, hot_here, free_pick)
    second = (first_pick + 1 + step_pick) % EXP_NODE
    node_ids = chosen.reshape(TOKENS, 3).astype(jnp.int32)
    local_ids = jnp.stack([first_pick, second], axis=-1).reshape(TOKENS, 6).astype(jnp.int32)
    return (node_ids, local_ids)


def draw_node_pick(key, part):
    return routing(key)[0]


def draw_expert_pick(key, part):
    return routing(key)[1]


def block_scale(own_key, extent, cuts, smallest, high):
    level, own = 1.0, jax.random.fold_in(own_key, 6)
    for axis_at, shards_of in cuts:
        heights = jnp.exp(jax.random.uniform(jax.random.fold_in(own, axis_at), (shards_of,), jnp.float32, smallest / len(cuts), high / len(cuts)))
        level = level * jnp.repeat(heights, extent[axis_at] // shards_of).reshape([-1 if axis == axis_at else 1 for axis in range(len(extent))])
    return level


def noise(stream_key, shape, width, reach, pieces=(), kind=jnp.bfloat16):
    gain = block_scale(stream_key, shape, pieces, -0.22, 0.18) if pieces else 1.0
    array = jax.random.normal(stream_key, shape, jnp.float32) * width * gain
    return jnp.minimum(jnp.maximum(array, -reach), reach).astype(kind)


def setup_inputs(seed: int = 0) -> dict:
    arg_keys = jax.random.split(jax.random.key(seed), 8)
    tokens = noise(arg_keys[0], (TOKENS, D), 1.0, 6.0, ((0, 32),))
    node_pick = draw_node_pick(jax.random.fold_in(arg_keys[7], 71), 0)
    expert_pick = draw_expert_pick(jax.random.fold_in(arg_keys[7], 71), 0)
    gate_weight = jnp.clip(jnp.exp(math.log(1.0) - 2.306499 * jax.random.uniform(arg_keys[3], (TOKENS, 6), jnp.float32) ** block_scale(arg_keys[3], (TOKENS, 6), ((0, 32),), -0.2, 0.2)), 0.099609375, 1.0).astype(jnp.bfloat16)
    w_gate = noise(arg_keys[4], (EXPERTS * FF, D), D ** -0.5, 0.078125, ((0, 32),))
    w_up = noise(arg_keys[5], (EXPERTS * FF, D), D ** -0.5, 0.078125, ((0, 32),))
    w_down = noise(arg_keys[6], (EXPERTS * FF, D), FF ** -0.5, 0.21875, ((0, 32),))
    return {"tokens": tokens, "node_pick": node_pick, "expert_pick": expert_pick, "gate_weight": gate_weight, "w_gate": w_gate, "w_up": w_up, "w_down": w_down}


def reference(tokens, node_pick, expert_pick, gate_weight, w_gate, w_up, w_down):
    owner_node = jnp.take(node_pick, jnp.arange(6, dtype=jnp.int32) // 2, axis=1)
    expert_ids = (owner_node * EXP_NODE + expert_pick).reshape(-1)
    capacity = N_DEV * CB
    slices = N_DEV // EXP_NODE
    ff_dev = FF // slices

    def per_expert(expert_index, running):
        is_hit = expert_ids == expert_index
        found_idx = jnp.nonzero(is_hit, size=capacity, fill_value=0)[0].astype(jnp.int32)
        is_valid = jnp.arange(capacity) < jnp.sum(is_hit.astype(jnp.int32))
        token_rows = jnp.take(tokens, found_idx // 6, axis=0)
        row_start = (expert_index * FF).astype(jnp.int32)
        gate_rows = lax.dynamic_slice_in_dim(w_gate, row_start, FF, 0)
        up_rows = lax.dynamic_slice_in_dim(w_up, row_start, FF, 0)
        down_rows = lax.dynamic_slice_in_dim(w_down, row_start, FF, 0)
        dims = (((1,), (1,)), ((), ()))
        gate_act = lax.dot_general(token_rows, gate_rows, dims, preferred_element_type=jnp.float32)
        up_act = lax.dot_general(token_rows, up_rows, dims, preferred_element_type=jnp.float32)
        hidden = (jax.nn.silu(gate_act) * up_act).astype(jnp.bfloat16)
        partial_value = jnp.einsum("csf,sfd->csd",
                             hidden.reshape(capacity, slices, ff_dev).astype(jnp.float32),
                             down_rows.reshape(slices, ff_dev, D).astype(jnp.float32),
                             precision=lax.Precision.HIGHEST)
        rounded = lax.optimization_barrier(partial_value.astype(jnp.bfloat16))
        expert_out = jnp.sum(rounded.astype(jnp.float32), axis=1)
        expert_out = jnp.where(is_valid[:, None], expert_out, jnp.float32(0.0))
        return running.at[found_idx].add(expert_out)

    running = lax.fori_loop(0, EXPERTS, per_expert, jnp.zeros((TOKENS * 6, D), jnp.float32))
    per_pick = running.reshape(TOKENS, 3, 2, D)
    weights = gate_weight.astype(jnp.float32).reshape(TOKENS, 3, 2, 1)
    node_part = jnp.sum(weights * per_pick, axis=2).astype(jnp.bfloat16)
    return jnp.sum(node_part.astype(jnp.float32), axis=1).astype(jnp.bfloat16)
```

```python
import functools

import jax
import jax.numpy as jnp
from jax import lax
from jax.experimental import pallas as pl
from jax.experimental.pallas import tpu as pltpu
from jax.sharding import PartitionSpec as P

EXP_NODE = 4


def plain_form(tokens, node_pick, expert_pick, gate_weight, w_gate, w_up, w_down):
    node_count = lax.axis_size("node")
    dev_count = lax.axis_size("dev")
    tok_rows = tokens.shape[0]
    feature_dim = tokens.shape[1]
    slot_count = 3 * tok_rows
    cycle_len = min(node_count, max(3, slot_count // 2))
    node_cap = (slot_count + cycle_len - 1) // cycle_len
    slices = dev_count // EXP_NODE
    node_slots = node_count * node_cap
    dest_node = node_pick.reshape(slot_count)
    slot_order = jnp.arange(slot_count, dtype=jnp.int32)
    earlier = (dest_node[:, None] == dest_node[None, :]) & (
        slot_order[None, :] < slot_order[:, None]
    )
    slot_rank = jnp.sum(earlier.astype(jnp.int32), axis=1)
    position = dest_node * node_cap + slot_rank
    place_table = (jnp.arange(node_slots, dtype=jnp.int32)[:, None] == position[None, :]).astype(
        jnp.bfloat16
    )
    local_pick = expert_pick.reshape(tok_rows, 3, 2)
    weights = gate_weight.reshape(tok_rows, 3, 2).astype(jnp.float32)
    chosen = (local_pick[..., None] == jnp.arange(EXP_NODE, dtype=jnp.int32)).astype(jnp.float32)
    slot_meta = (
        jnp.sum(weights[..., None] * chosen, axis=2)
        .reshape(slot_count, EXP_NODE)
        .astype(jnp.bfloat16)
    )
    sent_rows = jnp.dot(
        place_table, jnp.repeat(tokens, 3, axis=0), preferred_element_type=jnp.float32
    )
    sent_meta = jnp.dot(place_table, slot_meta, preferred_element_type=jnp.float32)
    sent_rows = sent_rows.astype(jnp.bfloat16).reshape(node_count, node_cap, feature_dim)
    sent_meta = sent_meta.astype(jnp.bfloat16).reshape(node_count, node_cap, EXP_NODE)
    got_rows, got_meta = (
        lax.all_to_all(sent_rows, "node", split_axis=0, concat_axis=0, tiled=True),
        lax.all_to_all(sent_meta, "node", split_axis=0, concat_axis=0, tiled=True),
    )
    got_rows = got_rows.reshape(node_slots, feature_dim)
    got_meta = got_meta.reshape(node_slots, EXP_NODE)
    is_live = got_meta > 0
    live_rank = jnp.cumsum(is_live.astype(jnp.int32), axis=0) - 1
    cap_ids = jnp.arange(slot_count, dtype=jnp.int32)[None, :, None]
    pick_table = is_live.T[:, None, :] & (live_rank.T[:, None, :] == cap_ids)
    pick_table = pick_table.reshape(EXP_NODE * slot_count, node_slots)
    packed = jnp.dot(
        pick_table.astype(jnp.bfloat16), got_rows, preferred_element_type=jnp.float32
    ).astype(jnp.bfloat16)
    outgoing = jnp.broadcast_to(
        packed.reshape(EXP_NODE, 1, slot_count, feature_dim),
        (EXP_NODE, slices, slot_count, feature_dim),
    ).reshape(dev_count, slot_count, feature_dim)
    arrived = lax.all_to_all(outgoing, "dev", split_axis=0, concat_axis=0, tiled=True)
    item_count = arrived.shape[1]
    flat_rows = arrived.reshape(dev_count * item_count, feature_dim)
    dims = (((1,), (1,)), ((), ()))
    gate_act = lax.dot_general(flat_rows, w_gate, dims, preferred_element_type=jnp.float32)
    up_act = lax.dot_general(flat_rows, w_up, dims, preferred_element_type=jnp.float32)
    hidden = (jax.nn.silu(gate_act) * up_act).astype(jnp.bfloat16)
    partial_value = jnp.dot(hidden, w_down, preferred_element_type=jnp.float32).astype(jnp.bfloat16)
    partial_value = partial_value.reshape(dev_count, item_count, feature_dim)
    returned = lax.all_to_all(partial_value, "dev", split_axis=0, concat_axis=0, tiled=True)
    expert_out = jnp.sum(
        returned.astype(jnp.float32).reshape(EXP_NODE, slices, slot_count, feature_dim), axis=1
    )
    expert_out = expert_out.reshape(EXP_NODE * slot_count, feature_dim)
    combine = pick_table.T.astype(jnp.float32) * jnp.repeat(
        got_meta.astype(jnp.float32), slot_count, axis=1
    )
    node_out = jnp.dot(
        combine, expert_out, precision=lax.Precision.HIGHEST, preferred_element_type=jnp.float32
    )
    node_out = node_out.astype(jnp.bfloat16).reshape(node_count, node_cap, feature_dim)
    home_rows = lax.all_to_all(node_out, "node", split_axis=0, concat_axis=0, tiled=True).reshape(
        node_slots, feature_dim
    )
    per_slot = jnp.dot(place_table.T, home_rows, preferred_element_type=jnp.float32)
    return jnp.sum(per_slot.reshape(tok_rows, 3, feature_dim), axis=1).astype(jnp.bfloat16)


LANES = 128
MESH = pl.DeviceIdType.MESH
CHUNKS = 4
VMEM_BYTES = 60 * 1024 * 1024


def fused_kernel(
    sizes,
    tok_ref,
    node_ref,
    pick_ref,
    weight_ref,
    wg_hbm,
    wu_hbm,
    wd_hbm,
    out_ref,
    wg,
    wu,
    wd,
    ext,
    sent,
    got,
    stack,
    rows,
    gate,
    up,
    part_keep,
    part_out,
    part_in,
    node_sent,
    node_got,
    home,
    w_sem,
    go_send,
    go_recv,
    dev_send,
    dev_recv,
    red_send,
    red_recv,
    back_send,
    back_recv,
):
    nodes, devs, cap, chunks = sizes
    slots = nodes * cap
    tok_rows, width = tok_ref.shape
    step = width // chunks
    me_n, me_d = lax.axis_index("node"), lax.axis_index("dev")
    rounds = devs.bit_length() - 1
    flips = [1 << (rounds - 1 - i) for i in range(rounds)]

    def partner(flip):
        return me_d + flip * (1 - 2 * (me_d // flip % 2))

    def cols(c, meta=False):
        return pl.ds(c * step, step + (LANES if meta else 0))

    weight_copies = []
    for c in range(chunks):
        for i, (src, dst) in enumerate(((wg_hbm, wg), (wu_hbm, wu))):
            weight_copies.append(
                pltpu.make_async_copy(
                    src.at[:, cols(c)], dst.at[:, cols(c)], w_sem.at[i, c]
                )
            )
    for c in range(chunks):
        weight_copies.append(
            pltpu.make_async_copy(
                wd_hbm.at[:, cols(c)], wd.at[:, cols(c)], w_sem.at[2, c]
            )
        )
    for copy in weight_copies:
        copy.start()

    barrier = pltpu.get_barrier_semaphore()
    peers = [(lax.rem(me_n + j, nodes), me_d) for j in range(1, nodes)]
    peers += [(me_n, partner(flip)) for flip in flips]
    for peer in peers:
        pl.semaphore_signal(barrier, inc=1, device_id=peer, device_id_type=MESH)

    lane = lax.broadcasted_iota(jnp.int32, (tok_rows, LANES), 1)
    down = lax.broadcasted_iota(jnp.int32, (tok_rows, LANES), 0)
    picked = node_ref[...]
    hit = jnp.zeros((tok_rows, LANES), jnp.int32)
    for k in range(3):
        hit = hit + (picked[:, k : k + 1] == lane // cap).astype(jnp.int32)
    rank = jnp.zeros((tok_rows, LANES), jnp.int32)
    for t in range(tok_rows - 1):
        rank = rank + jnp.where(down > t, hit[t : t + 1, :], 0)
    table = ((hit > 0) & (rank == lane % cap) & (lane < slots)).astype(jnp.float32)
    local = pick_ref[...]
    weights = weight_ref[...].astype(jnp.float32)
    dense = jnp.zeros((tok_rows, LANES), jnp.float32)
    for j in range(6):
        expert = picked[:, j // 2 : j // 2 + 1] * EXP_NODE + local[:, j : j + 1]
        dense = dense + jnp.where(expert == lane, weights[:, j : j + 1], 0.0)
    ext[:, :width] = tok_ref[...]
    ext[:, width:] = dense.astype(jnp.bfloat16)
    table_t = jnp.transpose(
        jnp.concatenate([table, jnp.zeros((8 - tok_rows, LANES), jnp.float32)], axis=0)
    )[:slots, :tok_rows].astype(jnp.bfloat16)
    placed = jnp.dot(table_t, ext[...], preferred_element_type=jnp.float32)
    for n in range(nodes):
        sent[n] = placed[n * cap : (n + 1) * cap].astype(jnp.bfloat16)

    pl.semaphore_wait(barrier, len(peers))

    def node_copy(j, c, source, target, send_sem, recv_sem, where, arriving=False):
        peer = lax.rem(me_n + j, nodes)
        landed = lax.rem(me_n + nodes - j, nodes) if arriving else me_n
        return pltpu.make_async_remote_copy(
            src_ref=source.at[peer, :, where],
            dst_ref=target.at[landed, :, where],
            send_sem=send_sem.at[c, j],
            recv_sem=recv_sem.at[c, j],
            device_id=(peer, me_d),
            device_id_type=MESH,
        )

    def go(c, j, arriving=False):
        where = cols(c, c == chunks - 1)
        return node_copy(j, c, sent, got, go_send, go_recv, where, arriving)

    for c in range(chunks):
        for j in range(1, nodes):
            go(c, j).start()
    got[me_n] = sent[me_n]

    def spread(c, i):
        held = slots << i
        where = cols(c, c == chunks - 1)
        return pltpu.make_async_remote_copy(
            src_ref=rows.at[pl.ds(0, held), where],
            dst_ref=rows.at[pl.ds(held, held), where],
            send_sem=dev_send.at[c, i],
            recv_sem=dev_recv.at[c, i],
            device_id=(me_n, partner(flips[i])),
            device_id_type=MESH,
        )

    def gather(c, i):
        if i == 0:
            where = cols(c, c == chunks - 1)
            for j in range(1, nodes):
                go(c, j, True).wait_recv()
            for n in range(nodes):
                stack[n * cap : (n + 1) * cap, where] = got[n, :, where].astype(jnp.float32)
            rows[:slots, where] = stack[:, where].astype(jnp.bfloat16)
        else:
            spread(c, i - 1).wait_recv()
        if i < rounds:
            spread(c, i).start()

    dims = (((1,), (1,)), ((), ()))

    def project(c):
        spread(c, rounds - 1).wait_recv()
        weight_copies[2 * c].wait()
        weight_copies[2 * c + 1].wait()
        for acc, w in ((gate, wg), (up, wu)):
            term = lax.dot_general(
                rows[:, cols(c)], w[:, cols(c)], dims, preferred_element_type=jnp.float32
            )
            acc[...] = term if c == 0 else acc[...] + term

    for wave in range(chunks + rounds):
        for c in range(chunks):
            i = wave - c
            if 0 <= i < rounds:
                gather(c, i)
        if wave >= rounds:
            project(wave - rounds)

    g = gate[...]
    hidden = (g / (1.0 + jnp.exp(-g)) * up[...]).astype(jnp.bfloat16)
    total_rows = slots * devs
    meta = rows[:, width:].astype(jnp.float32)
    mine = me_n * EXP_NODE + me_d // (devs // EXP_NODE)
    meta_lane = lax.broadcasted_iota(jnp.int32, (total_rows, LANES), 1)
    scale = jnp.sum(jnp.where(meta_lane == mine, meta, 0.0), axis=1, keepdims=True)

    def reduce_copy(c, i):
        half = slots << i
        return pltpu.make_async_remote_copy(
            src_ref=part_out.at[pl.ds(half, half), cols(c)],
            dst_ref=part_in.at[pl.ds(half, half), cols(c)],
            send_sem=red_send.at[c, i],
            recv_sem=red_recv.at[c, i],
            device_id=(me_n, partner(flips[i])),
            device_id_type=MESH,
        )

    for c in range(chunks):
        weight_copies[2 * chunks + c].wait()
        part = jnp.dot(hidden, wd[:, cols(c)], preferred_element_type=jnp.float32) * scale
        half = total_rows // 2
        part_out[half:, cols(c)] = part[half:].astype(jnp.bfloat16)
        reduce_copy(c, rounds - 1).start()
        part_keep[:, cols(c)] = part[:half]

    def back(c, j, arriving=False):
        return node_copy(j, c, node_sent, node_got, back_send, back_recv, cols(c), arriving)

    for i in reversed(range(rounds)):
        half = slots << i
        for c in range(chunks):
            reduce_copy(c, i).wait_recv()
            total = part_keep[:half, cols(c)] + part_in[
                half : 2 * half, cols(c)
            ].astype(jnp.float32)
            if i > 0:
                low = half // 2
                part_out[low:half, cols(c)] = total[low:].astype(jnp.bfloat16)
                reduce_copy(c, i - 1).start()
                part_keep[:low, cols(c)] = total[:low]
            else:
                for n in range(nodes):
                    node_sent[n, :, cols(c)] = total[n * cap : (n + 1) * cap].astype(jnp.bfloat16)
                for j in range(1, nodes):
                    back(c, j).start()
                node_got[me_n, :, cols(c)] = node_sent[me_n, :, cols(c)]

    for c in range(chunks):
        for j in range(1, nodes):
            back(c, j, True).wait_recv()
        for n in range(nodes):
            home[n * cap : (n + 1) * cap, cols(c)] = node_got[n, :, cols(c)].astype(jnp.float32)
        mixed = jnp.dot(
            table[:, :slots].astype(jnp.bfloat16),
            home[:, cols(c)].astype(jnp.bfloat16),
            preferred_element_type=jnp.float32,
        )
        out_ref[:, cols(c)] = mixed.astype(jnp.bfloat16)

    for c in range(chunks):
        for j in range(1, nodes):
            go(c, j).wait_send()
            back(c, j).wait_send()
        for i in range(rounds):
            spread(c, i).wait_send()
            reduce_copy(c, i).wait_send()


def fused_form(
    nodes, devs, cap, tokens, node_pick, expert_pick, gate_weight, w_gate, w_up, w_down
):
    tok_rows, width = tokens.shape
    hidden = w_gate.shape[0]
    slots = nodes * cap
    total = slots * devs
    rounds = devs.bit_length() - 1
    bf16, f32 = jnp.bfloat16, jnp.float32
    dma = pltpu.SemaphoreType.DMA
    scratch = [
        pltpu.VMEM((hidden, width), bf16),
        pltpu.VMEM((hidden, width), bf16),
        pltpu.VMEM((hidden, width), bf16),
        pltpu.VMEM((tok_rows, width + LANES), bf16),
        pltpu.VMEM((nodes, cap, width + LANES), bf16),
        pltpu.VMEM((nodes, cap, width + LANES), bf16),
        pltpu.VMEM((slots, width + LANES), f32),
        pltpu.VMEM((total, width + LANES), bf16),
        pltpu.VMEM((total, hidden), f32),
        pltpu.VMEM((total, hidden), f32),
        pltpu.VMEM((total // 2, width), f32),
        pltpu.VMEM((total, width), bf16),
        pltpu.VMEM((total, width), bf16),
        pltpu.VMEM((nodes, cap, width), bf16),
        pltpu.VMEM((nodes, cap, width), bf16),
        pltpu.VMEM((slots, width), f32),
        dma((3, CHUNKS)),
        dma((CHUNKS, nodes)),
        dma((CHUNKS, nodes)),
        dma((CHUNKS, rounds)),
        dma((CHUNKS, rounds)),
        dma((CHUNKS, rounds)),
        dma((CHUNKS, rounds)),
        dma((CHUNKS, nodes)),
        dma((CHUNKS, nodes)),
    ]
    vmem = pl.BlockSpec(memory_space=pltpu.VMEM)
    hbm = pl.BlockSpec(memory_space=pl.ANY)
    return pl.pallas_call(
        functools.partial(fused_kernel, (nodes, devs, cap, CHUNKS)),
        out_shape=jax.ShapeDtypeStruct((tok_rows, width), bf16),
        in_specs=[vmem] * 4 + [hbm] * 3,
        out_specs=vmem,
        scratch_shapes=scratch,
        compiler_params=pltpu.CompilerParams(
            collective_id=0, has_side_effects=True, vmem_limit_bytes=VMEM_BYTES
        ),
    )(tokens, node_pick, expert_pick, gate_weight, w_gate, w_up, w_down)


def on_device(*operands):
    nodes, devs = lax.axis_size("node"), lax.axis_size("dev")
    tok_rows, width = operands[0].shape
    hidden = operands[4].shape[0]
    slot_count = 3 * tok_rows
    cycle_len = min(nodes, max(3, slot_count // 2))
    cap = (slot_count + cycle_len - 1) // cycle_len
    slots = nodes * cap
    total = slots * devs
    held = 6 * hidden * width + total * (8 * width + 8 * hidden) + 24 * slots * width
    fits = (
        held < VMEM_BYTES * 9 // 10
        and slots % 16 == 0
        and slots <= LANES
        and nodes * EXP_NODE <= LANES
        and devs & (devs - 1) == 0
        and devs % EXP_NODE == 0
        and tok_rows <= 8
        and width % (CHUNKS * LANES) == 0
    )
    if not fits:
        return plain_form(*operands)
    return fused_form(nodes, devs, cap, *operands)


def solution(mesh):
    in_specs = (
        P(("node", "dev"), None),
        P(("node", "dev"), None),
        P(("node", "dev"), None),
        P(("node", "dev"), None),
        P(("node", "dev"), None),
        P(("node", "dev"), None),
        P(("node", "dev"), None),
    )
    out_specs = P(("node", "dev"), None)
    return jax.shard_map(
        on_device, mesh=mesh, in_specs=in_specs, out_specs=out_specs, check_vma=False
    )
```

```python
import functools

import jax
import jax.numpy as jnp
from jax import lax
from jax.experimental import pallas as pl
from jax.experimental.pallas import tpu as pltpu
from jax.sharding import PartitionSpec as P

EXP_NODE = 4


def plain_form(tokens, node_pick, expert_pick, gate_weight, w_gate, w_up, w_down):
    node_count = lax.axis_size("node")
    dev_count = lax.axis_size("dev")
    tok_rows = tokens.shape[0]
    feature_dim = tokens.shape[1]
    slot_count = 3 * tok_rows
    cycle_len = min(node_count, max(3, slot_count // 2))
    node_cap = (slot_count + cycle_len - 1) // cycle_len
    slices = dev_count // EXP_NODE
    node_slots = node_count * node_cap
    dest_node = node_pick.reshape(slot_count)
    slot_order = jnp.arange(slot_count, dtype=jnp.int32)
    earlier = (dest_node[:, None] == dest_node[None, :]) & (
        slot_order[None, :] < slot_order[:, None]
    )
    slot_rank = jnp.sum(earlier.astype(jnp.int32), axis=1)
    position = dest_node * node_cap + slot_rank
    place_table = (jnp.arange(node_slots, dtype=jnp.int32)[:, None] == position[None, :]).astype(
        jnp.bfloat16
    )
    local_pick = expert_pick.reshape(tok_rows, 3, 2)
    weights = gate_weight.reshape(tok_rows, 3, 2).astype(jnp.float32)
    chosen = (local_pick[..., None] == jnp.arange(EXP_NODE, dtype=jnp.int32)).astype(jnp.float32)
    slot_meta = (
        jnp.sum(weights[..., None] * chosen, axis=2)
        .reshape(slot_count, EXP_NODE)
        .astype(jnp.bfloat16)
    )
    sent_rows = jnp.dot(
        place_table, jnp.repeat(tokens, 3, axis=0), preferred_element_type=jnp.float32
    )
    sent_meta = jnp.dot(place_table, slot_meta, preferred_element_type=jnp.float32)
    sent_rows = sent_rows.astype(jnp.bfloat16).reshape(node_count, node_cap, feature_dim)
    sent_meta = sent_meta.astype(jnp.bfloat16).reshape(node_count, node_cap, EXP_NODE)
    got_rows, got_meta = (
        lax.all_to_all(sent_rows, "node", split_axis=0, concat_axis=0, tiled=True),
        lax.all_to_all(sent_meta, "node", split_axis=0, concat_axis=0, tiled=True),
    )
    got_rows = got_rows.reshape(node_slots, feature_dim)
    got_meta = got_meta.reshape(node_slots, EXP_NODE)
    is_live = got_meta > 0
    live_rank = jnp.cumsum(is_live.astype(jnp.int32), axis=0) - 1
    cap_ids = jnp.arange(slot_count, dtype=jnp.int32)[None, :, None]
    pick_table = is_live.T[:, None, :] & (live_rank.T[:, None, :] == cap_ids)
    pick_table = pick_table.reshape(EXP_NODE * slot_count, node_slots)
    packed = jnp.dot(
        pick_table.astype(jnp.bfloat16), got_rows, preferred_element_type=jnp.float32
    ).astype(jnp.bfloat16)
    outgoing = jnp.broadcast_to(
        packed.reshape(EXP_NODE, 1, slot_count, feature_dim),
        (EXP_NODE, slices, slot_count, feature_dim),
    ).reshape(dev_count, slot_count, feature_dim)
    arrived = lax.all_to_all(outgoing, "dev", split_axis=0, concat_axis=0, tiled=True)
    item_count = arrived.shape[1]
    flat_rows = arrived.reshape(dev_count * item_count, feature_dim)
    dims = (((1,), (1,)), ((), ()))
    gate_act = lax.dot_general(flat_rows, w_gate, dims, preferred_element_type=jnp.float32)
    up_act = lax.dot_general(flat_rows, w_up, dims, preferred_element_type=jnp.float32)
    hidden = (jax.nn.silu(gate_act) * up_act).astype(jnp.bfloat16)
    partial_value = jnp.dot(hidden, w_down, preferred_element_type=jnp.float32).astype(jnp.bfloat16)
    partial_value = partial_value.reshape(dev_count, item_count, feature_dim)
    returned = lax.all_to_all(partial_value, "dev", split_axis=0, concat_axis=0, tiled=True)
    expert_out = jnp.sum(
        returned.astype(jnp.float32).reshape(EXP_NODE, slices, slot_count, feature_dim), axis=1
    )
    expert_out = expert_out.reshape(EXP_NODE * slot_count, feature_dim)
    combine = pick_table.T.astype(jnp.float32) * jnp.repeat(
        got_meta.astype(jnp.float32), slot_count, axis=1
    )
    node_out = jnp.dot(
        combine, expert_out, precision=lax.Precision.HIGHEST, preferred_element_type=jnp.float32
    )
    node_out = node_out.astype(jnp.bfloat16).reshape(node_count, node_cap, feature_dim)
    home_rows = lax.all_to_all(node_out, "node", split_axis=0, concat_axis=0, tiled=True).reshape(
        node_slots, feature_dim
    )
    per_slot = jnp.dot(place_table.T, home_rows, preferred_element_type=jnp.float32)
    return jnp.sum(per_slot.reshape(tok_rows, 3, feature_dim), axis=1).astype(jnp.bfloat16)


LANES = 128
MESH = pl.DeviceIdType.MESH
CHUNKS = 1
VMEM_BYTES = 60 * 1024 * 1024


def fused_kernel(
    sizes,
    tok_ref,
    node_ref,
    pick_ref,
    weight_ref,
    wg_hbm,
    wu_hbm,
    wd_hbm,
    out_ref,
    wg,
    wu,
    wd,
    ext,
    sent,
    got,
    stack,
    rows,
    gate,
    up,
    part_keep,
    part_out,
    part_in,
    node_sent,
    node_got,
    home,
    w_sem,
    go_send,
    go_recv,
    dev_send,
    dev_recv,
    red_send,
    red_recv,
    back_send,
    back_recv,
):
    nodes, devs, cap, chunks = sizes
    slots = nodes * cap
    tok_rows, width = tok_ref.shape
    step = width // chunks
    me_n, me_d = lax.axis_index("node"), lax.axis_index("dev")
    rounds = devs.bit_length() - 1
    flips = [1 << (rounds - 1 - i) for i in range(rounds)]

    def partner(flip):
        return me_d + flip * (1 - 2 * (me_d // flip % 2))

    def cols(c, meta=False):
        return pl.ds(c * step, step + (LANES if meta else 0))

    weight_copies = []
    for c in range(chunks):
        for i, (src, dst) in enumerate(((wg_hbm, wg), (wu_hbm, wu))):
            weight_copies.append(
                pltpu.make_async_copy(
                    src.at[:, cols(c)], dst.at[:, cols(c)], w_sem.at[i, c]
                )
            )
    for c in range(chunks):
        weight_copies.append(
            pltpu.make_async_copy(
                wd_hbm.at[:, cols(c)], wd.at[:, cols(c)], w_sem.at[2, c]
            )
        )
    for copy in weight_copies:
        copy.start()

    barrier = pltpu.get_barrier_semaphore()
    peers = [(lax.rem(me_n + j, nodes), me_d) for j in range(1, nodes)]
    peers += [(me_n, partner(flip)) for flip in flips]
    for peer in peers:
        pl.semaphore_signal(barrier, inc=1, device_id=peer, device_id_type=MESH)

    lane = lax.broadcasted_iota(jnp.int32, (tok_rows, LANES), 1)
    down = lax.broadcasted_iota(jnp.int32, (tok_rows, LANES), 0)
    picked = node_ref[...]
    hit = jnp.zeros((tok_rows, LANES), jnp.int32)
    for k in range(3):
        hit = hit + (picked[:, k : k + 1] == lane // cap).astype(jnp.int32)
    rank = jnp.zeros((tok_rows, LANES), jnp.int32)
    for t in range(tok_rows - 1):
        rank = rank + jnp.where(down > t, hit[t : t + 1, :], 0)
    table = ((hit > 0) & (rank == lane % cap) & (lane < slots)).astype(jnp.float32)
    local = pick_ref[...]
    weights = weight_ref[...].astype(jnp.float32)
    dense = jnp.zeros((tok_rows, LANES), jnp.float32)
    for j in range(6):
        expert = picked[:, j // 2 : j // 2 + 1] * EXP_NODE + local[:, j : j + 1]
        dense = dense + jnp.where(expert == lane, weights[:, j : j + 1], 0.0)
    ext[:, :width] = tok_ref[...]
    ext[:, width:] = dense.astype(jnp.bfloat16)
    table_t = jnp.transpose(
        jnp.concatenate([table, jnp.zeros((8 - tok_rows, LANES), jnp.float32)], axis=0)
    )[:slots, :tok_rows].astype(jnp.bfloat16)
    placed = jnp.dot(table_t, ext[...], preferred_element_type=jnp.float32)
    for n in range(nodes):
        sent[n] = placed[n * cap : (n + 1) * cap].astype(jnp.bfloat16)

    pl.semaphore_wait(barrier, len(peers))

    def node_copy(j, c, source, target, send_sem, recv_sem, where, arriving=False):
        peer = lax.rem(me_n + j, nodes)
        landed = lax.rem(me_n + nodes - j, nodes) if arriving else me_n
        return pltpu.make_async_remote_copy(
            src_ref=source.at[peer, :, where],
            dst_ref=target.at[landed, :, where],
            send_sem=send_sem.at[c, j],
            recv_sem=recv_sem.at[c, j],
            device_id=(peer, me_d),
            device_id_type=MESH,
        )

    def go(c, j, arriving=False):
        where = cols(c, c == chunks - 1)
        return node_copy(j, c, sent, got, go_send, go_recv, where, arriving)

    for c in range(chunks):
        for j in range(1, nodes):
            go(c, j).start()
    got[me_n] = sent[me_n]

    def spread(c, i):
        held = slots << i
        where = cols(c, c == chunks - 1)
        return pltpu.make_async_remote_copy(
            src_ref=rows.at[pl.ds(0, held), where],
            dst_ref=rows.at[pl.ds(held, held), where],
            send_sem=dev_send.at[c, i],
            recv_sem=dev_recv.at[c, i],
            device_id=(me_n, partner(flips[i])),
            device_id_type=MESH,
        )

    def gather(c, i):
        if i == 0:
            where = cols(c, c == chunks - 1)
            for j in range(1, nodes):
                go(c, j, True).wait_recv()
            for n in range(nodes):
                stack[n * cap : (n + 1) * cap, where] = got[n, :, where].astype(jnp.float32)
            rows[:slots, where] = stack[:, where].astype(jnp.bfloat16)
        else:
            spread(c, i - 1).wait_recv()
        if i < rounds:
            spread(c, i).start()

    dims = (((1,), (1,)), ((), ()))

    def project(c):
        spread(c, rounds - 1).wait_recv()
        weight_copies[2 * c].wait()
        weight_copies[2 * c + 1].wait()
        for acc, w in ((gate, wg), (up, wu)):
            term = lax.dot_general(
                rows[:, cols(c)], w[:, cols(c)], dims, preferred_element_type=jnp.float32
            )
            acc[...] = term if c == 0 else acc[...] + term

    for wave in range(chunks + rounds):
        for c in range(chunks):
            i = wave - c
            if 0 <= i < rounds:
                gather(c, i)
        if wave >= rounds:
            project(wave - rounds)

    g = gate[...]
    hidden = (g / (1.0 + jnp.exp(-g)) * up[...]).astype(jnp.bfloat16)
    total_rows = slots * devs
    meta = rows[:, width:].astype(jnp.float32)
    mine = me_n * EXP_NODE + me_d // (devs // EXP_NODE)
    meta_lane = lax.broadcasted_iota(jnp.int32, (total_rows, LANES), 1)
    scale = jnp.sum(jnp.where(meta_lane == mine, meta, 0.0), axis=1, keepdims=True)

    def reduce_copy(c, i):
        half = slots << i
        return pltpu.make_async_remote_copy(
            src_ref=part_out.at[pl.ds(half, half), cols(c)],
            dst_ref=part_in.at[pl.ds(half, half), cols(c)],
            send_sem=red_send.at[c, i],
            recv_sem=red_recv.at[c, i],
            device_id=(me_n, partner(flips[i])),
            device_id_type=MESH,
        )

    for c in range(chunks):
        weight_copies[2 * chunks + c].wait()
        part = jnp.dot(hidden, wd[:, cols(c)], preferred_element_type=jnp.float32) * scale
        half = total_rows // 2
        part_out[half:, cols(c)] = part[half:].astype(jnp.bfloat16)
        reduce_copy(c, rounds - 1).start()
        part_keep[:, cols(c)] = part[:half]

    def back(c, j, arriving=False):
        return node_copy(j, c, node_sent, node_got, back_send, back_recv, cols(c), arriving)

    for i in reversed(range(rounds)):
        half = slots << i
        for c in range(chunks):
            reduce_copy(c, i).wait_recv()
            total = part_keep[:half, cols(c)] + part_in[
                half : 2 * half, cols(c)
            ].astype(jnp.float32)
            if i > 0:
                low = half // 2
                part_out[low:half, cols(c)] = total[low:].astype(jnp.bfloat16)
                reduce_copy(c, i - 1).start()
                part_keep[:low, cols(c)] = total[:low]
            else:
                for n in range(nodes):
                    node_sent[n, :, cols(c)] = total[n * cap : (n + 1) * cap].astype(jnp.bfloat16)
                for j in range(1, nodes):
                    back(c, j).start()
                node_got[me_n, :, cols(c)] = node_sent[me_n, :, cols(c)]

    for c in range(chunks):
        for j in range(1, nodes):
            back(c, j, True).wait_recv()
        for n in range(nodes):
            home[n * cap : (n + 1) * cap, cols(c)] = node_got[n, :, cols(c)].astype(jnp.float32)
        mixed = jnp.dot(
            table[:, :slots].astype(jnp.bfloat16),
            home[:, cols(c)].astype(jnp.bfloat16),
            preferred_element_type=jnp.float32,
        )
        out_ref[:, cols(c)] = mixed.astype(jnp.bfloat16)

    for c in range(chunks):
        for j in range(1, nodes):
            go(c, j).wait_send()
            back(c, j).wait_send()
        for i in range(rounds):
            spread(c, i).wait_send()
            reduce_copy(c, i).wait_send()


def fused_form(
    nodes, devs, cap, tokens, node_pick, expert_pick, gate_weight, w_gate, w_up, w_down
):
    tok_rows, width = tokens.shape
    hidden = w_gate.shape[0]
    slots = nodes * cap
    total = slots * devs
    rounds = devs.bit_length() - 1
    bf16, f32 = jnp.bfloat16, jnp.float32
    dma = pltpu.SemaphoreType.DMA
    scratch = [
        pltpu.VMEM((hidden, width), bf16),
        pltpu.VMEM((hidden, width), bf16),
        pltpu.VMEM((hidden, width), bf16),
        pltpu.VMEM((tok_rows, width + LANES), bf16),
        pltpu.VMEM((nodes, cap, width + LANES), bf16),
        pltpu.VMEM((nodes, cap, width + LANES), bf16),
        pltpu.VMEM((slots, width + LANES), f32),
        pltpu.VMEM((total, width + LANES), bf16),
        pltpu.VMEM((total, hidden), f32),
        pltpu.VMEM((total, hidden), f32),
        pltpu.VMEM((total // 2, width), f32),
        pltpu.VMEM((total, width), bf16),
        pltpu.VMEM((total, width), bf16),
        pltpu.VMEM((nodes, cap, width), bf16),
        pltpu.VMEM((nodes, cap, width), bf16),
        pltpu.VMEM((slots, width), f32),
        dma((3, CHUNKS)),
        dma((CHUNKS, nodes)),
        dma((CHUNKS, nodes)),
        dma((CHUNKS, rounds)),
        dma((CHUNKS, rounds)),
        dma((CHUNKS, rounds)),
        dma((CHUNKS, rounds)),
        dma((CHUNKS, nodes)),
        dma((CHUNKS, nodes)),
    ]
    vmem = pl.BlockSpec(memory_space=pltpu.VMEM)
    hbm = pl.BlockSpec(memory_space=pl.ANY)
    return pl.pallas_call(
        functools.partial(fused_kernel, (nodes, devs, cap, CHUNKS)),
        out_shape=jax.ShapeDtypeStruct((tok_rows, width), bf16),
        in_specs=[vmem] * 4 + [hbm] * 3,
        out_specs=vmem,
        scratch_shapes=scratch,
        compiler_params=pltpu.CompilerParams(
            collective_id=0, has_side_effects=True, vmem_limit_bytes=VMEM_BYTES
        ),
    )(tokens, node_pick, expert_pick, gate_weight, w_gate, w_up, w_down)


def on_device(*operands):
    nodes, devs = lax.axis_size("node"), lax.axis_size("dev")
    tok_rows, width = operands[0].shape
    hidden = operands[4].shape[0]
    slot_count = 3 * tok_rows
    cycle_len = min(nodes, max(3, slot_count // 2))
    cap = (slot_count + cycle_len - 1) // cycle_len
    slots = nodes * cap
    total = slots * devs
    held = 6 * hidden * width + total * (8 * width + 8 * hidden) + 24 * slots * width
    fits = (
        held < VMEM_BYTES * 9 // 10
        and slots % 16 == 0
        and slots <= LANES
        and nodes * EXP_NODE <= LANES
        and devs & (devs - 1) == 0
        and devs % EXP_NODE == 0
        and tok_rows <= 8
        and width % (CHUNKS * LANES) == 0
    )
    if not fits:
        return plain_form(*operands)
    return fused_form(nodes, devs, cap, *operands)


def solution(mesh):
    in_specs = (
        P(("node", "dev"), None),
        P(("node", "dev"), None),
        P(("node", "dev"), None),
        P(("node", "dev"), None),
        P(("node", "dev"), None),
        P(("node", "dev"), None),
        P(("node", "dev"), None),
    )
    out_specs = P(("node", "dev"), None)
    return jax.shard_map(
        on_device, mesh=mesh, in_specs=in_specs, out_specs=out_specs, check_vma=False
    )
```
